256 devices in a mesh: seq: 64 (over z, y, core), comp: 4 (over x).
Axes of the slice: x: 4, y: 4, z: 8, core: 2. Of those that a mesh axis runs over, the one named last changes fastest.
Arguments:
- points: float32 [131072, 256], P('seq'), may hold values from -6 to 6
- assign: int32 [64, 2048], P('seq'), may hold values from 0 to 3, never falling along the last dimension, each value on 1 to 1024 neighbouring positions
- plan: int32 [64, 4], P('seq'), may hold values from 64 to 255
- init_mass: float32 [1024], P('comp'), may hold values from 0.00024414062 to 0.00390625
- init_means: float32 [1024, 256], P('comp'), may hold values from -3 to 3
- init_vars: float32 [1024, 256], P('comp'), may hold values from 0.5 to 2
Outputs:
- dev_logmass: float32 [64, 1024], P('seq', 'comp')
- dev_means: float32 [64, 1024, 256], P('seq', 'comp')
- dev_vars: float32 [64, 1024, 256], P('seq', 'comp')
- final_logmass: float32 [64, 1024], P('seq', 'comp')
- final_means: float32 [64, 1024, 256], P('seq', 'comp')
- final_vars: float32 [64, 1024, 256], P('seq', 'comp')
The draws below stay inside these ranges and needn't reach their ends.
Inputs may be any that keep to these rules, and one draw needn't show every extreme that they name: `assign`: in each row, minibatch numbers never fall along the row and every minibatch has at least one point.
All inputs are finite; a program needn't handle non-finite values.
Results may differ from the reference program's by a relative error of at most 0.0003.
Values sent between devices are 32-bit elements; how exact they have to be, the bound alone decides.
A program may use at most 64 MiB of HBM per device.

```python
import math
import jax
import jax.numpy as jnp
import numpy as np
from jax import lax

D = 256
K = 1024
MB_DEV = 4
PTS_DEV = 2048
POINTS = 131072
MINIBATCHES = 256
N_SEQ = 64


def with_ends(entries, rng, low, largest):
    shape = entries.shape
    spot = [jax.random.randint(jax.random.fold_in(rng, axis), (), 0, shape[axis]) for axis in range(len(shape))]
    entries = entries.at[tuple(spot)].set(low)
    longest = shape.index(max(shape))
    spot[longest] = (spot[longest] + 1) % shape[longest]
    return entries.at[tuple(spot)].set(largest)


def levels(stream_key, extent, split, low, top_value):
    def one(axis_at, blocks):
        steps = jax.random.uniform(jax.random.fold_in(jax.random.fold_in(stream_key, 6), axis_at), (blocks,), jnp.float32, low / len(split), top_value / len(split))
        return jnp.repeat(jnp.exp(steps), extent[axis_at] // blocks).reshape((-1,) + (1,) * (len(extent) - axis_at - 1))

    gain = one(*split[0])
    for cut in split[1:]:
        gain = gain * one(*cut)
    return gain


def profile(count, total, reach, lean):
    loads = [(1 << 20) // math.isqrt(rank ** lean) + 1 for rank in range(2, count + 1)]
    rest, holding = total - reach - (count - 1), [1] * (count - 1)
    while rest > 0:
        free = [i for i in range(count - 1) if holding[i] < reach]
        mass, remaining = sum([loads[i] for i in free]), rest
        for i in free:
            extra = min(reach - holding[i], max(1, remaining * loads[i] // mass), rest)
            holding[i] = holding[i] + extra
            rest = rest - extra
    return np.array([reach] + holding)


def uneven(key, amount, total, reach, skew):
    if amount == 2:
        one = jax.random.randint(key, (), max(1, total - reach), min(reach, total - 1) + 1)
        return jnp.stack([one, total - one])
    sizes = jnp.asarray(profile(amount, total, reach, skew), jnp.int32)
    pairs = (amount - 1) // 2
    donor, taker = sizes[1:1 + 2 * pairs:2], sizes[2:2 + 2 * pairs:2]
    margin = jnp.minimum(donor - 1, reach - taker)
    passed = jax.random.randint(jax.random.fold_in(key, 1), (pairs,), 0, 1 << 20) % (margin + 1)
    sizes = sizes.at[1:1 + 2 * pairs:2].set(donor - passed).at[2:2 + 2 * pairs:2].set(taker + passed)
    return sizes[jax.random.permutation(jax.random.fold_in(key, 2), amount)]


def centred(rng, shape, deviation, limit, shards=(), kind=jnp.bfloat16):
    result = deviation * jax.random.normal(rng, shape, jnp.float32)
    if shards:
        result = result * levels(rng, shape, shards, -0.22, 0.18)
    return jnp.clip(result, -limit, limit).astype(kind)


def setup_inputs(seed: int = 0) -> dict:
    arg_keys = jax.random.split(jax.random.key(seed), 7)
    return {
        "points": centred(arg_keys[0], (POINTS, D), 1.0, 6.0, ((0, 64),), jnp.float32),
        "assign": jax.vmap(lambda own: jnp.searchsorted(jnp.cumsum(uneven(own, MB_DEV, PTS_DEV, min(PTS_DEV, 2 * PTS_DEV // MB_DEV), 1)), jnp.arange(PTS_DEV), side="right"))(jax.random.split(arg_keys[1], N_SEQ)).reshape((N_SEQ, PTS_DEV)).astype(jnp.int32),
        "plan": with_ends(jax.random.randint(arg_keys[2], (N_SEQ, MB_DEV), MINIBATCHES // 4, MINIBATCHES), jax.random.fold_in(arg_keys[2], 1), MINIBATCHES // 4, MINIBATCHES - 1).astype(jnp.int32),
        "init_mass": jnp.clip(jnp.exp(math.log(0.00390625) - 2.7725887 * jax.random.uniform(arg_keys[3], (K,), jnp.float32) ** levels(arg_keys[3], (K,), ((0, 4),), -0.2, 0.2)), 0.00024414062, 0.00390625),
        "init_means": centred(arg_keys[4], (K, D), 0.5, 3.0, ((0, 4),), jnp.float32),
        "init_vars": jnp.clip(jnp.exp(math.log(2.0) - 1.3862944 * jax.random.uniform(arg_keys[5], (K, D), jnp.float32) ** levels(arg_keys[5], (K, D), ((0, 4),), -0.2, 0.2)), 0.5, 2.0),
    }


VAR_PRIOR = 0.01
best_precision = lax.Precision.HIGHEST


def prepare(init_mass, init_means, init_vars):
    inverse = 1.0 / init_vars
    lookup = jnp.concatenate([init_means * inverse, -0.5 * inverse], axis=1)
    offsets = jnp.log(init_mass) - 0.5 * jnp.sum(jnp.log(init_vars) + init_means * init_means * inverse, axis=1)
    start_moment = jnp.concatenate([init_mass[:, None] * init_means, init_mass[:, None] * (init_vars + init_means * init_means)], axis=1)
    return lookup, offsets, start_moment


def point_weights(assign_row, plan_row):
    step_size = 1.0 / plan_row.astype(jnp.float32)
    retain = 1.0 - step_size
    inclusive = jnp.flip(jnp.cumprod(jnp.flip(retain)))
    later_keep = jnp.concatenate([inclusive[1:], jnp.ones((1,), jnp.float32)])
    onehot = (assign_row[:, None] == jnp.arange(MB_DEV, dtype=jnp.int32)[None, :]).astype(jnp.float32)
    counts = jnp.sum(onehot, axis=0)
    batch_weight = step_size * later_keep / counts
    return jnp.sum(onehot * batch_weight[None, :], axis=1), inclusive[0]


def maximize(mass_stat, moment_stat):
    half_width = moment_stat.shape[1] // 2
    centers = moment_stat[:, :half_width] / mass_stat[:, None]
    spreads = moment_stat[:, half_width:] / mass_stat[:, None] - centers * centers + VAR_PRIOR
    return jnp.log(mass_stat), centers, spreads


def reference(points, assign, plan, init_mass, init_means, init_vars):
    lookup, offsets, start_moment = prepare(init_mass, init_means, init_vars)
    blocks = points.reshape(N_SEQ, PTS_DEV, D)

    def advance(state_pair, inputs):
        mass_stat, moment_stat = state_pair
        coords, assign_row, plan_row = inputs
        features = jnp.concatenate([coords, coords * coords], axis=1)
        logits = lax.dot_general(features, lookup, (((1,), (1,)), ((), ())), precision=best_precision, preferred_element_type=jnp.float32) + offsets[None, :]
        row_peak = jnp.max(logits, axis=1, keepdims=True)
        exponent = jnp.exp(logits - row_peak)
        responsibility = exponent / jnp.sum(exponent, axis=1, keepdims=True)
        weight_row, decay_all = point_weights(assign_row, plan_row)
        weighted = responsibility * weight_row[:, None]
        mass_term = jnp.sum(weighted, axis=0)
        moment_term = lax.dot_general(weighted, features, (((0,), (0,)), ((), ())), precision=best_precision, preferred_element_type=jnp.float32)
        mass_stat = decay_all * mass_stat + mass_term
        moment_stat = decay_all * moment_stat + moment_term
        return (mass_stat, moment_stat), maximize(mass_stat, moment_stat)

    final_state, outputs = lax.scan(advance, (init_mass, start_moment), (blocks, assign, plan))
    final_logmass, final_means, final_vars = maximize(final_state[0], final_state[1])
    every_logmass = jnp.broadcast_to(final_logmass[None], (N_SEQ,) + final_logmass.shape)
    every_means = jnp.broadcast_to(final_means[None], (N_SEQ,) + final_means.shape)
    every_vars = jnp.broadcast_to(final_vars[None], (N_SEQ,) + final_vars.shape)
    return outputs[0], outputs[1], outputs[2], every_logmass, every_means, every_vars
```

```python
import functools

import jax
import jax.numpy as jnp
from jax import lax
from jax.experimental import pallas as pl
from jax.experimental.pallas import tpu as pltpu
from jax.sharding import Mesh
from jax.sharding import PartitionSpec as P

SEQ = ("seq_0", "seq_1", "seq_2")
MESH = pl.DeviceIdType.MESH
VAR_PRIOR = 0.01
BLOCK = 512


def split3(a):
    hi = a.astype(jnp.bfloat16)
    rest = a - hi.astype(jnp.float32)
    mid = rest.astype(jnp.bfloat16)
    low = (rest - mid.astype(jnp.float32)).astype(jnp.bfloat16)
    return hi, mid, low


def dot_nt(a, b):
    return lax.dot_general(a, b, (((1,), (1,)), ((), ())), preferred_element_type=jnp.float32)


def dot_nn(a, b):
    return lax.dot_general(a, b, (((1,), (0,)), ((), ())), preferred_element_type=jnp.float32)


def drain(ref, sem):
    pltpu.make_async_copy(ref, ref, sem).wait()


def kernel(
    nz, ny, nx,
    pts, asg, plan, mass_in, means, varis,
    dlog, dmean, dvar, flog, fmean, fvar,
    look, feat1, feat2, expo, wsplit, wrow, mcol,
    stat, statin, mine, other, partner, pair_small, small, smallbuf,
    term, inbuf, outbuf, carrybuf, total, state, stateout,
    x_send, x_recv, pair_send, pair_recv, in_send, in_recv, sm_send, sm_recv,
    carry_send, carry_recv, t1_send, t1_recv, t2_send, t2_recv,
):
    z, y, c, x = (lax.axis_index(n) for n in (*SEQ, "comp"))
    nc = nz * ny
    kl, width = means.shape
    share = kl // nc
    blocks = pts.shape[0] // BLOCK
    here = z * ny + y
    own = y * nz + z

    def owned(q):
        return lax.rem(q, ny) * nz + q // ny

    def chip(q):
        return {"seq_0": q // ny, "seq_1": lax.rem(q, ny)}

    def rows(o):
        return pl.ds(pl.multiple_of(o * share, share), share)

    mate = {"seq_2": 1 - c}

    barrier = pltpu.get_barrier_semaphore()

    @pl.loop(1, nc)
    def _(k):
        pl.semaphore_signal(barrier, inc=1, device_id=chip(lax.rem(here + k, nc)), device_id_type=MESH)

    pl.semaphore_signal(barrier, inc=1, device_id=mate, device_id_type=MESH)
    for k in range(1, nx):
        pl.semaphore_signal(barrier, inc=1, device_id={"comp": lax.rem(x + k, nx)}, device_id_type=MESH)

    mu, var = means[...], varis[...]
    inverse = 1.0 / var
    for h, table in enumerate((mu * inverse, -0.5 * inverse)):
        for part, piece in enumerate(split3(table)):
            look[part, :, h * width : (h + 1) * width] = piece
    diagonal = lax.broadcasted_iota(jnp.int32, (kl, kl), 0) == lax.broadcasted_iota(jnp.int32, (kl, kl), 1)

    def column(row):
        return jnp.sum(jnp.where(diagonal, row, 0.0), axis=1, keepdims=True)

    def row_of(col):
        return jnp.sum(jnp.where(diagonal, col, 0.0), axis=0, keepdims=True)

    start_col = column(mass_in[...])
    mcol[...] = jnp.broadcast_to(start_col, mcol.shape)
    offset = jnp.log(start_col) - 0.5 * jnp.sum(jnp.log(var) + mu * mu * inverse, axis=1, keepdims=True)

    steps = 1.0 / plan[...].astype(jnp.float32)
    keep = jnp.ones((1, 1), jnp.float32)
    weight = jnp.zeros(asg.shape, jnp.float32)
    for m in range(plan.shape[1] - 1, -1, -1):
        step = steps[:, m : m + 1]
        chosen = asg[...] == m
        count = jnp.sum(jnp.where(chosen, 1.0, 0.0), axis=1, keepdims=True)
        weight = jnp.where(chosen, step * keep / count, weight)
        keep = keep * (1.0 - step)
    decay_row = jnp.broadcast_to(keep, (1, kl))
    for b in range(blocks):
        wrow[b] = weight[:, b * BLOCK : (b + 1) * BLOCK]

    for b in range(blocks):
        p = pts[b * BLOCK : (b + 1) * BLOCK, :]
        logits = None
        thirds = []
        for h, f in enumerate((p, p * p)):
            hi, mid, low = split3(f)
            feat1[h, b] = hi
            feat2[h, b] = mid
            thirds.append((hi, mid, low))
        hi, mid, low = (jnp.concatenate([thirds[0][i], thirds[1][i]], axis=1) for i in range(3))
        logits = dot_nt(hi, look[2]) + dot_nt(low, look[0]) + dot_nt(mid, look[1])
        logits = logits + dot_nt(hi, look[1]) + dot_nt(mid, look[0]) + dot_nt(hi, look[0])
        logits = logits.T + offset
        peak = jnp.max(logits, axis=0, keepdims=True)
        e = jnp.exp(logits - peak)
        expo[b] = e
        stat[b, 0:1, :] = peak
        stat[b, 1:2, :] = jnp.sum(e, axis=0, keepdims=True)
        if b == 0:
            pl.semaphore_wait(barrier, nc - 1 + 1 + nx - 1)
        for k in range(1, nx):
            pltpu.make_async_remote_copy(
                stat.at[b], statin.at[k - 1, b], x_send.at[k - 1, b], x_recv.at[k - 1, b],
                device_id={"comp": lax.rem(x + k, nx)}, device_id_type=MESH,
            ).start()

    mass = jnp.zeros((kl, 1), jnp.float32)
    acc = jnp.zeros((kl, width), jnp.float32)
    for b in range(blocks):
        for k in range(1, nx):
            pltpu.make_async_remote_copy(
                stat.at[b], statin.at[k - 1, b], x_send.at[k - 1, b], x_recv.at[k - 1, b],
                device_id={"comp": lax.rem(x + k, nx)}, device_id_type=MESH,
            ).wait()
        near = stat[b, 0:1, :]
        peaks = [near] + [statin[k, b, 0:1, :] for k in range(nx - 1)]
        sums = [stat[b, 1:2, :]] + [statin[k, b, 1:2, :] for k in range(nx - 1)]
        peak = functools.reduce(jnp.maximum, peaks)
        whole = sum(s * jnp.exp(q - peak) for q, s in zip(peaks, sums))
        scale = jnp.exp(near - peak) / whole * wrow[b]
        w = expo[b] * scale
        mass = mass + jnp.sum(w, axis=1, keepdims=True)
        w1 = w.astype(jnp.bfloat16)
        w2 = (w - w1.astype(jnp.float32)).astype(jnp.bfloat16)
        wsplit[0, b] = w1
        wsplit[1, b] = w2
        f1, f2 = feat1[1 - c, b], feat2[1 - c, b]
        acc = acc + dot_nn(w2, f1) + dot_nn(w1, f2) + dot_nn(w1, f1)
    other[...] = acc
    to_mate = pltpu.make_async_remote_copy(
        other, partner, pair_send.at[0], pair_recv.at[0], device_id=mate, device_id_type=MESH
    )
    to_mate.start()
    pair_small[c, 0:1, :] = row_of(mass)
    pair_small[c, 1:2, :] = decay_row
    small_mate = pltpu.make_async_remote_copy(
        pair_small.at[c], pair_small.at[c], pair_send.at[1], pair_recv.at[1], device_id=mate, device_id_type=MESH
    )
    small_mate.start()
    acc = jnp.zeros((kl, width), jnp.float32)
    for b in range(blocks):
        w1, w2 = wsplit[0, b], wsplit[1, b]
        f1, f2 = feat1[c, b], feat2[c, b]
        acc = acc + dot_nn(w2, f1) + dot_nn(w1, f2) + dot_nn(w1, f1)
    mine[...] = acc
    small_mate.wait()
    to_mate.wait()

    first_core = c == 0
    decay0, decay1 = pair_small[0, 1:2, :], pair_small[1, 1:2, :]
    one = jnp.ones_like(decay0)
    term[...] = jnp.where(first_core, decay1, one) * acc + jnp.where(first_core, one, decay1) * partner[...]
    small[0:1, :] = decay1 * pair_small[0, 0:1, :] + pair_small[1, 0:1, :]
    small[1:2, :] = decay0 * decay1

    @pl.loop(1, nc)
    def _(k):
        q = lax.rem(here + k, nc)
        pltpu.make_async_remote_copy(
            small, smallbuf.at[here], sm_send, sm_recv, device_id=chip(q), device_id_type=MESH
        ).start()
        pltpu.make_async_remote_copy(
            term.at[rows(owned(q))], inbuf.at[here], in_send, in_recv, device_id=chip(q), device_id_type=MESH
        ).start()

    inbuf[here] = term[rows(own), :]
    smallbuf[here] = small[...]
    mu_own, var_own = means[rows(own), :], varis[rows(own), :]
    s = mcol[rows(own), 0:1] * jnp.where(first_core, mu_own, var_own + mu_own * mu_own)
    ms = mass_in[...]
    drain(smallbuf.at[pl.ds(0, nc - 1)], sm_recv)
    drain(inbuf.at[pl.ds(0, nc - 1)], in_recv)

    def advance(q, held):
        s, ms, entry = held
        entry = jnp.where(q == here, ms, entry)
        outbuf[q] = s
        decay = smallbuf[q, 1:2, :]
        return decay * s + inbuf[q], decay * ms + smallbuf[q, 0:1, :], entry

    s, ms, entry_mass = lax.fori_loop(0, nc, advance, (s, ms, ms), unroll=4)
    total[c, rows(own), :] = s

    for k in range(1, nz):
        pltpu.make_async_remote_copy(
            total.at[c, rows(own)], total.at[c, rows(own)], t1_send, t1_recv,
            device_id={"seq_0": lax.rem(z + k, nz)}, device_id_type=MESH,
        ).start()

    @pl.loop(1, nc)
    def _(k):
        q = lax.rem(here + k, nc)
        pltpu.make_async_remote_copy(
            outbuf.at[q], carrybuf.at[rows(own)], carry_send, carry_recv, device_id=chip(q), device_id_type=MESH
        ).start()

    carrybuf[rows(own), :] = outbuf[here]
    drain(total.at[0, pl.ds(0, (nz - 1) * share)], t1_recv)
    line = pl.ds(pl.multiple_of(y * nz * share, nz * share), nz * share)
    for k in range(1, ny):
        pltpu.make_async_remote_copy(
            total.at[c, line], total.at[c, line], t2_send, t2_recv,
            device_id={"seq_1": lax.rem(y + k, ny)}, device_id_type=MESH,
        ).start()
    drain(total.at[0, pl.ds(0, (ny - 1) * nz * share)], t2_recv)
    total_mate = pltpu.make_async_remote_copy(
        total.at[c], total.at[c], pair_send.at[2], pair_recv.at[2], device_id=mate, device_id_type=MESH
    )
    total_mate.start()

    drain(carrybuf.at[pl.ds(0, (nc - 1) * share)], carry_recv)
    from_own, from_mate = mine[...], partner[...]
    state0 = decay0 * carrybuf[...] + jnp.where(first_core, from_own, from_mate)
    state1 = decay1 * state0 + jnp.where(first_core, from_mate, from_own)
    stateout[...] = jnp.where(first_core, state1, state0)
    state_mate = pltpu.make_async_remote_copy(
        stateout, state.at[c], pair_send.at[3], pair_recv.at[3], device_id=mate, device_id_type=MESH
    )
    state_mate.start()
    state[c] = jnp.where(first_core, state0, state1)
    mass0 = decay0 * entry_mass + pair_small[0, 0:1, :]
    mass1 = decay1 * mass0 + pair_small[1, 0:1, :]
    mass_row = jnp.where(first_core, mass0, mass1)
    dlog[...] = jnp.log(mass_row)
    flog[...] = jnp.log(ms)
    inv_dev, inv_final = 1.0 / column(mass_row), 1.0 / column(ms)

    total_mate.wait()
    centers = total[0] * inv_final
    fmean[...] = centers
    fvar[...] = total[1] * inv_final - centers * centers + VAR_PRIOR
    state_mate.wait()
    centers = state[0] * inv_dev
    dmean[...] = centers
    dvar[...] = state[1] * inv_dev - centers * centers + VAR_PRIOR

    drain(smallbuf.at[pl.ds(0, nc - 1)], sm_send)
    drain(inbuf.at[pl.ds(0, nc - 1)], in_send)
    drain(carrybuf.at[pl.ds(0, (nc - 1) * share)], carry_send)
    drain(total.at[0, pl.ds(0, (nz - 1) * share)], t1_send)
    drain(total.at[0, pl.ds(0, (ny - 1) * nz * share)], t2_send)


def local(nz, ny, nx, points, assign, plan, init_mass, init_means, init_vars):
    kl, width = init_means.shape
    count = points.shape[0]
    nc, blocks = nz * ny, count // BLOCK
    share = kl // nc
    f32, bf16 = jnp.float32, jnp.bfloat16
    vmem, dma = pltpu.VMEM, pltpu.SemaphoreType.DMA
    row, table = jax.ShapeDtypeStruct((1, kl), f32), jax.ShapeDtypeStruct((kl, width), f32)
    outs = pl.pallas_call(
        functools.partial(kernel, nz, ny, nx),
        out_shape=(row, table, table, row, table, table),
        in_specs=[pl.BlockSpec(memory_space=vmem)] * 6,
        out_specs=[pl.BlockSpec(memory_space=vmem)] * 6,
        scratch_shapes=[
            vmem((3, kl, 2 * width), bf16),
            vmem((2, blocks, BLOCK, width), bf16),
            vmem((2, blocks, BLOCK, width), bf16),
            vmem((blocks, kl, BLOCK), f32),
            vmem((2, blocks, kl, BLOCK), bf16),
            vmem((blocks, 1, BLOCK), f32),
            vmem((kl, 128), f32),
            vmem((blocks, 2, BLOCK), f32),
            vmem((nx - 1, blocks, 2, BLOCK), f32),
            vmem((kl, width), f32),
            vmem((kl, width), f32),
            vmem((kl, width), f32),
            vmem((2, 2, kl), f32),
            vmem((2, kl), f32),
            vmem((nc, 2, kl), f32),
            vmem((kl, width), f32),
            vmem((nc, share, width), f32),
            vmem((nc, share, width), f32),
            vmem((kl, width), f32),
            vmem((2, kl, width), f32),
            vmem((2, kl, width), f32),
            vmem((kl, width), f32),
            dma((nx - 1, blocks)), dma((nx - 1, blocks)),
            dma((4,)), dma((4,)),
            dma, dma, dma, dma, dma, dma, dma, dma, dma, dma,
        ],
        compiler_params=pltpu.CompilerParams(collective_id=0, has_side_effects=True, vmem_limit_bytes=60 * 2**20),
    )(points, assign, plan, init_mass.reshape(1, kl), init_means, init_vars)
    return tuple(o.reshape(1, kl) if o.shape[0] == 1 else o[None] for o in outs)


def solution(mesh):
    nz, ny, nx = 8, 4, mesh.shape["comp"]
    split = Mesh(mesh.devices.reshape(nz, ny, 2, nx), (*SEQ, "comp"))
    return jax.shard_map(
        functools.partial(local, nz, ny, nx),
        mesh=split,
        in_specs=(P(SEQ, None), P(SEQ, None), P(SEQ, None), P("comp"), P("comp", None), P("comp", None)),
        out_specs=(
            P(SEQ, "comp"), P(SEQ, "comp", None), P(SEQ, "comp", None),
            P(SEQ, "comp"), P(SEQ, "comp", None), P(SEQ, "comp", None),
        ),
        check_vma=False,
    )
```

```python
import functools

import jax
import jax.numpy as jnp
from jax import lax
from jax.experimental import pallas as pl
from jax.experimental.pallas import tpu as pltpu
from jax.sharding import Mesh
from jax.sharding import PartitionSpec as P

SEQ = ("seq_0", "seq_1", "seq_2")
MESH = pl.DeviceIdType.MESH
VAR_PRIOR = 0.01
BLOCK = 512


def split3(a):
    hi = a.astype(jnp.bfloat16)
    rest = a - hi.astype(jnp.float32)
    mid = rest.astype(jnp.bfloat16)
    low = (rest - mid.astype(jnp.float32)).astype(jnp.bfloat16)
    return hi, mid, low


def dot_nt(a, b):
    return lax.dot_general(a, b, (((1,), (1,)), ((), ())), preferred_element_type=jnp.float32)


def dot_nn(a, b):
    return lax.dot_general(a, b, (((1,), (0,)), ((), ())), preferred_element_type=jnp.float32)


def drain(ref, sem):
    pltpu.make_async_copy(ref, ref, sem).wait()


def kernel(
    nz, ny, nx,
    pts_in, asg_in, plan_in, mass_from, means_in, varis_in,
    dlog, dmean, dvar, flog, fmean, fvar,
    pts, means, varis, asg, plan, mass_in, load,
    look, feat1, feat2, expo, wsplit, wrow, mcol,
    stat, statin, mine, other, partner, pair_decay, pair_mass, decay, decays, mass_out, masses,
    term, inbuf, outbuf, carrybuf, total, state, stateout,
    x_send, x_recv, pair_send, pair_recv, in_send, in_recv, mass_send, mass_recv, decay_send, decay_recv,
    carry_send, carry_recv, t1_send, t1_recv, t2_send, t2_recv,
):
    loads = [
        pltpu.make_async_copy(means_in, means, load.at[0]),
        pltpu.make_async_copy(varis_in, varis, load.at[1]),
        pltpu.make_async_copy(mass_from, mass_in, load.at[2]),
        pltpu.make_async_copy(asg_in, asg, load.at[3]),
        pltpu.make_async_copy(plan_in, plan, load.at[4]),
    ] + [
        pltpu.make_async_copy(pts_in.at[pl.ds(b * BLOCK, BLOCK)], pts.at[b], load.at[5 + b]) for b in range(pts.shape[0])
    ]
    for copy in loads:
        copy.start()
    z, y, c, x = (lax.axis_index(n) for n in (*SEQ, "comp"))
    nc = nz * ny
    kl, width = means.shape
    share = kl // nc
    blocks = pts.shape[0]
    here = z * ny + y
    own = y * nz + z

    def owned(q):
        return lax.rem(q, ny) * nz + q // ny

    def chip(q):
        return {"seq_0": q // ny, "seq_1": lax.rem(q, ny)}

    def rows(o):
        return pl.ds(pl.multiple_of(o * share, share), share)

    mate = {"seq_2": 1 - c}

    def away(offset, size):
        return min(offset, size - offset)

    offsets = [(dz, dy) for dz in range(nz) for dy in range(ny) if dz or dy]

    offsets.sort(key=lambda d: away(d[0], nz) + away(d[1], ny))
    others = [lax.rem(z + dz, nz) * ny + lax.rem(y + dy, ny) for dz, dy in offsets]

    barrier = pltpu.get_barrier_semaphore()

    @pl.loop(1, nc)
    def _(k):
        pl.semaphore_signal(barrier, inc=1, device_id=chip(lax.rem(here + k, nc)), device_id_type=MESH)

    pl.semaphore_signal(barrier, inc=1, device_id=mate, device_id_type=MESH)
    for k in range(1, nx):
        pl.semaphore_signal(barrier, inc=1, device_id={"comp": lax.rem(x + k, nx)}, device_id_type=MESH)

    for k in range(5):
        loads[k].wait()
    mu, var = means[...], varis[...]
    inverse = 1.0 / var
    for h, table in enumerate((mu * inverse, -0.5 * inverse)):
        for part, piece in enumerate(split3(table.T)):
            look[part, h * width : (h + 1) * width, :] = piece
    diagonal = lax.broadcasted_iota(jnp.int32, (kl, kl), 0) == lax.broadcasted_iota(jnp.int32, (kl, kl), 1)

    def column(row):
        return jnp.sum(jnp.where(diagonal, row, 0.0), axis=1, keepdims=True)

    def row_of(col):
        return jnp.sum(jnp.where(diagonal, col, 0.0), axis=0, keepdims=True)

    start_col = column(mass_in[...])
    mcol[...] = jnp.broadcast_to(start_col, mcol.shape)
    offset = jnp.log(start_col) - 0.5 * jnp.sum(jnp.log(var) + mu * mu * inverse, axis=1, keepdims=True)

    steps = 1.0 / plan[...].astype(jnp.float32)
    keep = jnp.ones((1, 1), jnp.float32)
    weight = jnp.zeros(asg.shape, jnp.float32)
    for m in range(plan.shape[1] - 1, -1, -1):
        step = steps[:, m : m + 1]
        chosen = asg[...] == m
        count = jnp.sum(jnp.where(chosen, 1.0, 0.0), axis=1, keepdims=True)
        weight = jnp.where(chosen, step * keep / count, weight)
        keep = keep * (1.0 - step)
    pair_decay[c] = jnp.broadcast_to(keep, (1, kl))
    for b in range(blocks):
        wrow[b] = weight[:, b * BLOCK : (b + 1) * BLOCK]

    def stats_to_peers(b):
        return [
            pltpu.make_async_remote_copy(
                stat.at[b], statin.at[k - 1, b], x_send.at[k - 1, b], x_recv.at[k - 1, b],
                device_id={"comp": lax.rem(x + k, nx)}, device_id_type=MESH,
            )
            for k in range(1, nx)
        ]

    for b in range(blocks):
        loads[5 + b].wait()
    decay_mate = pltpu.make_async_remote_copy(
        pair_decay.at[c], pair_decay.at[c], pair_send.at[4], pair_recv.at[4], device_id=mate, device_id_type=MESH
    )
    early = max(blocks - 1, 1)
    for b in range(blocks):
        p = pts[b]
        first, second = split3(p), split3(p * p)
        for h, f in enumerate((first, second)):
            feat1[h, b] = f[0]
            feat2[h, b] = f[1]
        hi, mid, low = (jnp.concatenate([first[i], second[i]], axis=1) for i in range(3))
        halves = []
        for r in range(2):
            part = slice(r * (BLOCK // 2), (r + 1) * (BLOCK // 2))
            logits = dot_nn(hi[part], look[2]) + dot_nn(low[part], look[0]) + dot_nn(mid[part], look[1])
            logits = logits + dot_nn(hi[part], look[1]) + dot_nn(mid[part], look[0]) + dot_nn(hi[part], look[0])
            halves.append(logits.T + offset)
        logits = jnp.concatenate(halves, axis=1)
        peak = jnp.max(logits, axis=0, keepdims=True)
        e = jnp.exp(logits - peak)
        expo[b] = e
        stat[b, 0:1, :] = peak
        stat[b, 1:2, :] = jnp.sum(e, axis=0, keepdims=True)
        if b == early - 1:
            pl.semaphore_wait(barrier, nc - 1 + 1 + nx - 1)
            decay_mate.start()
            for ready in range(early):
                for copy in stats_to_peers(ready):
                    copy.start()
        if b >= early:
            for copy in stats_to_peers(b):
                copy.start()
    decay_mate.wait()
    decay0, decay1 = pair_decay[0], pair_decay[1]
    decay[...] = decay0 * decay1
    decays[here] = decay0 * decay1
    for q in others:
        pltpu.make_async_remote_copy(
            decay, decays.at[here], decay_send, decay_recv, device_id=chip(q), device_id_type=MESH
        ).start()

    half = kl // 2
    mass = jnp.zeros((kl, 1), jnp.float32)

    def moments(held, h, b):
        return [
            (coarse + dot_nn(wsplit[b, a], feat1[h, b]), fine + dot_nn(wsplit[b, a, 0:half, :], feat2[h, b]))
            for a, (coarse, fine) in enumerate(held)
        ]

    def nothing():
        return [(jnp.zeros((kl, width), jnp.float32), jnp.zeros((half, width), jnp.float32))] * 2

    def summed(held):
        return jnp.concatenate([fine + coarse[half:] + coarse[:half] for coarse, fine in held], axis=0)

    held = nothing()
    for b in range(blocks):
        if b % 2 == 0:
            for copy in stats_to_peers(b) + stats_to_peers(b + 1):
                copy.wait()
        near = stat[b, 0:1, :]
        peaks = [near] + [statin[k, b, 0:1, :] for k in range(nx - 1)]
        sums = [stat[b, 1:2, :]] + [statin[k, b, 1:2, :] for k in range(nx - 1)]
        peak = functools.reduce(jnp.maximum, peaks)
        whole = sum(s * jnp.exp(q - peak) for q, s in zip(peaks, sums))
        scale = jnp.exp(near - peak) / whole * wrow[b]
        w = expo[b] * scale
        mass = mass + jnp.sum(w, axis=1, keepdims=True)
        w1 = w.astype(jnp.bfloat16)
        w2 = (w - w1.astype(jnp.float32)).astype(jnp.bfloat16)
        for a in range(2):
            wsplit[b, a, 0:half, :] = w1[a * half : (a + 1) * half]
            wsplit[b, a, half:kl, :] = w2[a * half : (a + 1) * half]
        held = moments(held, 1 - c, b)
    other[...] = summed(held)
    to_mate = pltpu.make_async_remote_copy(
        other, partner, pair_send.at[0], pair_recv.at[0], device_id=mate, device_id_type=MESH
    )
    to_mate.start()
    pair_mass[c] = row_of(mass)
    mass_mate = pltpu.make_async_remote_copy(
        pair_mass.at[c], pair_mass.at[c], pair_send.at[1], pair_recv.at[1], device_id=mate, device_id_type=MESH
    )
    mass_mate.start()
    held = nothing()
    for b in range(blocks):
        held = moments(held, c, b)
    acc = summed(held)
    mine[...] = acc
    to_mate.wait()

    first_core = c == 0
    one = jnp.ones_like(decay0)
    term[...] = jnp.where(first_core, decay1, one) * acc + jnp.where(first_core, one, decay1) * partner[...]
    for q in others:
        pltpu.make_async_remote_copy(
            term.at[rows(owned(q))], inbuf.at[here], in_send, in_recv, device_id=chip(q), device_id_type=MESH
        ).start()
    mass_mate.wait()
    mass_out[...] = decay1 * pair_mass[0] + pair_mass[1]
    masses[here] = mass_out[...]
    for q in others:
        pltpu.make_async_remote_copy(
            mass_out, masses.at[here], mass_send, mass_recv, device_id=chip(q), device_id_type=MESH
        ).start()
    inbuf[here] = term[rows(own), :]
    mu_own, var_own = means[rows(own), :], varis[rows(own), :]
    s = mcol[rows(own), 0:1] * jnp.where(first_core, mu_own, var_own + mu_own * mu_own)
    drain(decays.at[pl.ds(0, nc - 1)], decay_recv)
    drain(inbuf.at[pl.ds(0, nc - 1)], in_recv)

    def advance(q, s):
        outbuf[q] = s
        return decays[q] * s + inbuf[q]

    s = lax.fori_loop(0, nc, advance, s, unroll=4)
    total[c, rows(own), :] = s

    for k in range(1, nz):
        pltpu.make_async_remote_copy(
            total.at[c, rows(own)], total.at[c, rows(own)], t1_send, t1_recv,
            device_id={"seq_0": lax.rem(z + k, nz)}, device_id_type=MESH,
        ).start()

    for q in others:
        pltpu.make_async_remote_copy(
            outbuf.at[q], carrybuf.at[rows(own)], carry_send, carry_recv, device_id=chip(q), device_id_type=MESH
        ).start()

    carrybuf[rows(own), :] = outbuf[here]

    drain(masses.at[pl.ds(0, nc - 1)], mass_recv)

    def mass_step(q, held):
        ms, entry = held
        entry = jnp.where(q == here, ms, entry)
        return decays[q] * ms + masses[q], entry

    ms, entry_mass = lax.fori_loop(0, nc, mass_step, (mass_in[...], mass_in[...]), unroll=4)

    def lines(row):
        return pl.ds(pl.multiple_of(row * nz * share, nz * share), nz * share)

    def line_to_mate(row):
        return pltpu.make_async_remote_copy(
            total.at[c, lines(row)], total.at[c, lines(row)], pair_send.at[2], pair_recv.at[2],
            device_id=mate, device_id_type=MESH,
        )

    drain(total.at[0, pl.ds(0, (nz - 1) * share)], t1_recv)
    for k in range(1, ny):
        pltpu.make_async_remote_copy(
            total.at[c, lines(y)], total.at[c, lines(y)], t2_send, t2_recv.at[k - 1],
            device_id={"seq_1": lax.rem(y + k, ny)}, device_id_type=MESH,
        ).start()
    line_to_mate(y).start()

    drain(carrybuf.at[pl.ds(0, (nc - 1) * share)], carry_recv)
    from_own, from_mate = mine[...], partner[...]
    state0 = decay0 * carrybuf[...] + jnp.where(first_core, from_own, from_mate)
    state1 = decay1 * state0 + jnp.where(first_core, from_mate, from_own)
    stateout[...] = jnp.where(first_core, state1, state0)
    state_mate = pltpu.make_async_remote_copy(
        stateout, state.at[c], pair_send.at[3], pair_recv.at[3], device_id=mate, device_id_type=MESH
    )
    state_mate.start()
    state[c] = jnp.where(first_core, state0, state1)
    for k in range(1, ny):
        drain(total.at[0, pl.ds(0, nz * share)], t2_recv.at[k - 1])
        line_to_mate(lax.rem(y - k + ny, ny)).start()
    mass0 = decay0 * entry_mass + pair_mass[0]
    mass1 = decay1 * mass0 + pair_mass[1]
    mass_row = jnp.where(first_core, mass0, mass1)
    dlog[...] = jnp.log(mass_row)
    flog[...] = jnp.log(ms)
    inv_dev, inv_final = 1.0 / column(mass_row), 1.0 / column(ms)

    state_mate.wait()
    centers = state[0] * inv_dev
    dmean[...] = centers
    dvar[...] = state[1] * inv_dev - centers * centers + VAR_PRIOR
    drain(total.at[0], pair_recv.at[2])
    centers = total[0] * inv_final
    fmean[...] = centers
    fvar[...] = total[1] * inv_final - centers * centers + VAR_PRIOR

    drain(total.at[0], pair_send.at[2])
    drain(masses.at[pl.ds(0, nc - 1)], mass_send)
    drain(decays.at[pl.ds(0, nc - 1)], decay_send)
    drain(inbuf.at[pl.ds(0, nc - 1)], in_send)
    drain(carrybuf.at[pl.ds(0, (nc - 1) * share)], carry_send)
    drain(total.at[0, pl.ds(0, (nz - 1) * share)], t1_send)
    drain(total.at[0, pl.ds(0, (ny - 1) * nz * share)], t2_send)


def deliver(*refs):
    copies = [pltpu.make_async_copy(refs[k], refs[6 + k], refs[12].at[k]) for k in range(6)]
    for copy in copies:
        copy.start()
    for copy in copies:
        copy.wait()


def local(nz, ny, nx, points, assign, plan, init_mass, init_means, init_vars):
    kl, width = init_means.shape
    count = points.shape[0]
    nc, blocks = nz * ny, count // BLOCK
    share = kl // nc
    f32, bf16 = jnp.float32, jnp.bfloat16
    vmem, hbm, dma = pltpu.VMEM, pltpu.HBM, pltpu.SemaphoreType.DMA
    row, table = jax.ShapeDtypeStruct((1, kl), f32), jax.ShapeDtypeStruct((kl, width), f32)
    far = functools.partial(pltpu.with_memory_space_constraint, memory_space=hbm)
    outs = pl.pallas_call(
        functools.partial(kernel, nz, ny, nx),
        out_shape=(row, table, table, row, table, table),
        in_specs=[pl.BlockSpec(memory_space=hbm)] * 6,
        out_specs=[pl.BlockSpec(memory_space=vmem)] * 6,
        scratch_shapes=[
            vmem((blocks, BLOCK, width), f32),
            vmem((kl, width), f32),
            vmem((kl, width), f32),
            vmem((1, count), jnp.int32),
            vmem(plan.shape, jnp.int32),
            vmem((1, kl), f32),
            dma((5 + blocks,)),
            vmem((3, 2 * width, kl), bf16),
            vmem((2, blocks, BLOCK, width), bf16),
            vmem((2, blocks, BLOCK, width), bf16),
            vmem((blocks, kl, BLOCK), f32),
            vmem((blocks, 2, kl, BLOCK), bf16),
            vmem((blocks, 1, BLOCK), f32),
            vmem((kl, 128), f32),
            vmem((blocks, 2, BLOCK), f32),
            vmem((nx - 1, blocks, 2, BLOCK), f32),
            vmem((kl, width), f32),
            vmem((kl, width), f32),
            vmem((kl, width), f32),
            vmem((2, 1, kl), f32),
            vmem((2, 1, kl), f32),
            vmem((1, kl), f32),
            vmem((nc, 1, kl), f32),
            vmem((1, kl), f32),
            vmem((nc, 1, kl), f32),
            vmem((kl, width), f32),
            vmem((nc, share, width), f32),
            vmem((nc, share, width), f32),
            vmem((kl, width), f32),
            vmem((2, kl, width), f32),
            vmem((2, kl, width), f32),
            vmem((kl, width), f32),
            dma((nx - 1, blocks)), dma((nx - 1, blocks)),
            dma((5,)), dma((5,)),
            dma, dma, dma, dma, dma, dma, dma, dma, dma, dma, dma, dma((ny - 1,)),
        ],
        compiler_params=pltpu.CompilerParams(collective_id=0, has_side_effects=True, vmem_limit_bytes=32 * 2**20),
    )(*(far(a) for a in (points, assign, plan, init_mass.reshape(1, kl), init_means, init_vars)))
    outs = pl.pallas_call(
        deliver,
        out_shape=tuple(jax.ShapeDtypeStruct(o.shape, f32) for o in outs),
        in_specs=[pl.BlockSpec(memory_space=vmem)] * 6,
        out_specs=[pl.BlockSpec(memory_space=hbm)] * 6,
        scratch_shapes=[dma((6,))],
        compiler_params=pltpu.CompilerParams(vmem_limit_bytes=2 * 2**20),
    )(*outs)
    return tuple(o.reshape(1, kl) if o.shape[0] == 1 else o[None] for o in outs)


def solution(mesh):
    nz, ny, nx = 8, 4, mesh.shape["comp"]
    split = Mesh(mesh.devices.reshape(nz, ny, 2, nx), (*SEQ, "comp"))
    return jax.shard_map(
        functools.partial(local, nz, ny, nx),
        mesh=split,
        in_specs=(P(SEQ, None), P(SEQ, None), P(SEQ, None), P("comp"), P("comp", None), P("comp", None)),
        out_specs=(
            P(SEQ, "comp"), P(SEQ, "comp", None), P(SEQ, "comp", None),
            P(SEQ, "comp"), P(SEQ, "comp", None), P(SEQ, "comp", None),
        ),
        check_vma=False,
    )
```

```python
import functools

import jax
import jax.numpy as jnp
from jax import lax
from jax.experimental import pallas as pl
from jax.experimental.pallas import tpu as pltpu
from jax.sharding import Mesh
from jax.sharding import PartitionSpec as P

SEQ = ("seq_0", "seq_1", "seq_2")
MESH = pl.DeviceIdType.MESH
VAR_PRIOR = 0.01
BLOCK = 512
PARTS = 2


def split3(a):
    hi = a.astype(jnp.bfloat16)
    rest = a - hi.astype(jnp.float32)
    mid = rest.astype(jnp.bfloat16)
    low = (rest - mid.astype(jnp.float32)).astype(jnp.bfloat16)
    return hi, mid, low


def dot_nt(a, b):
    return lax.dot_general(a, b, (((1,), (1,)), ((), ())), preferred_element_type=jnp.float32)


def dot_nn(a, b):
    return lax.dot_general(a, b, (((1,), (0,)), ((), ())), preferred_element_type=jnp.float32)


def drain(ref, sem):
    pltpu.make_async_copy(ref, ref, sem).wait()


def kernel(
    nz, ny, nx,
    pts_in, asg_in, plan_in, mass_from, means_in, varis_in,
    dlog, dmean, dvar, flog, fmean, fvar,
    pts, means, varis, asg, plan, mass_in, load,
    look, feat1, feat2, expo, wsplit, wrow, mcol,
    stat, statin, mine, other, partner, pair_decay, pair_mass, decay_y, decay_z, mass_y, mass_z,
    term, terms, before, plane, planes, entry, entries, lines, linein, state, stateout, mystate, total,
    inv_dev, inv_final,
    x_send, x_recv, pair_send, pair_recv, term_send, term_recv, plane_send, plane_recv, entry_send, entry_recv,
    line_send, line_recv, decay_send, decay_recv, mass_send, mass_recv, chunk_send, chunk_recv,
):
    loads = [
        pltpu.make_async_copy(means_in, means, load.at[0]),
        pltpu.make_async_copy(varis_in, varis, load.at[1]),
        pltpu.make_async_copy(mass_from, mass_in, load.at[2]),
        pltpu.make_async_copy(asg_in, asg, load.at[3]),
        pltpu.make_async_copy(plan_in, plan, load.at[4]),
    ] + [
        pltpu.make_async_copy(pts_in.at[pl.ds(b * BLOCK, BLOCK)], pts.at[b], load.at[5 + b]) for b in range(pts.shape[0])
    ]
    for copy in loads:
        copy.start()
    z, y, c, x = (lax.axis_index(n) for n in (*SEQ, "comp"))
    nc = nz * ny
    kl, width = means.shape
    share = kl // nc
    blocks = pts.shape[0]
    band = kl // ny
    mate = {"seq_2": 1 - c}

    def spread(size):
        near = sorted(range(1, size), key=lambda k: min(k, size - k))
        return [near[-1 - k // 2] if k % 2 == 0 else near[k // 2] for k in range(len(near))]

    def along_y(k):
        return lax.rem(y + k, ny)

    def along_z(k):
        return lax.rem(z + k, nz)

    def band_rows(q):
        return pl.ds(pl.multiple_of(q * band, band), band)

    def rows(q):
        return pl.ds(pl.multiple_of(q * share, share), share)

    def to_y(k, src, dst, send, recv):
        return pltpu.make_async_remote_copy(
            src, dst, send, recv, device_id={"seq_1": along_y(k)}, device_id_type=MESH
        )

    def to_z(k, src, dst, send, recv):
        return pltpu.make_async_remote_copy(
            src, dst, send, recv, device_id={"seq_0": along_z(k)}, device_id_type=MESH
        )

    def to_mate(src, dst, send, recv):
        return pltpu.make_async_remote_copy(src, dst, send, recv, device_id=mate, device_id_type=MESH)

    barrier = pltpu.get_barrier_semaphore()

    for k in range(1, nz):
        pl.semaphore_signal(barrier, inc=1, device_id={"seq_0": along_z(k)}, device_id_type=MESH)
    for k in range(1, ny):
        pl.semaphore_signal(barrier, inc=1, device_id={"seq_1": along_y(k)}, device_id_type=MESH)
    pl.semaphore_signal(barrier, inc=1, device_id=mate, device_id_type=MESH)
    for k in range(1, nx):
        pl.semaphore_signal(barrier, inc=1, device_id={"comp": lax.rem(x + k, nx)}, device_id_type=MESH)

    for k in range(5):
        loads[k].wait()
    mu, var = means[...], varis[...]
    inverse = 1.0 / var
    for h, table in enumerate((mu * inverse, -0.5 * inverse)):
        for part, piece in enumerate(split3(table.T)):
            look[part, h * width : (h + 1) * width, :] = piece
    diagonal = lax.broadcasted_iota(jnp.int32, (kl, kl), 0) == lax.broadcasted_iota(jnp.int32, (kl, kl), 1)

    def column(row):
        return jnp.sum(jnp.where(diagonal, row, 0.0), axis=1, keepdims=True)

    def row_of(col):
        return jnp.sum(jnp.where(diagonal, col, 0.0), axis=0, keepdims=True)

    start_col = column(mass_in[...])
    mcol[...] = jnp.broadcast_to(start_col, mcol.shape)
    offset = jnp.log(start_col) - 0.5 * jnp.sum(jnp.log(var) + mu * mu * inverse, axis=1, keepdims=True)

    steps = 1.0 / plan[...].astype(jnp.float32)
    keep = jnp.ones((1, 1), jnp.float32)
    weight = jnp.zeros(asg.shape, jnp.float32)
    for m in range(plan.shape[1] - 1, -1, -1):
        step = steps[:, m : m + 1]
        chosen = asg[...] == m
        count = jnp.sum(jnp.where(chosen, 1.0, 0.0), axis=1, keepdims=True)
        weight = jnp.where(chosen, step * keep / count, weight)
        keep = keep * (1.0 - step)
    pair_decay[c] = jnp.broadcast_to(keep, (1, kl))
    for b in range(blocks):
        wrow[b] = weight[:, b * BLOCK : (b + 1) * BLOCK]

    def stats_to_peers(b):
        return [
            pltpu.make_async_remote_copy(
                stat.at[b], statin.at[k - 1, b], x_send.at[k - 1, b], x_recv.at[k - 1, b],
                device_id={"comp": lax.rem(x + k, nx)}, device_id_type=MESH,
            )
            for k in range(1, nx)
        ]

    for b in range(blocks):
        loads[5 + b].wait()
    decay_mate = to_mate(pair_decay.at[c], pair_decay.at[c], pair_send.at[0], pair_recv.at[0])
    early = max(blocks - 1, 1)
    for b in range(blocks):
        p = pts[b]
        first, second = split3(p), split3(p * p)
        for h, f in enumerate((first, second)):
            feat1[h, b] = f[0]
            feat2[h, b] = f[1]
        hi, mid, low = (jnp.concatenate([first[i], second[i]], axis=1) for i in range(3))
        halves = []
        for r in range(2):
            part = slice(r * (BLOCK // 2), (r + 1) * (BLOCK // 2))
            logits = dot_nn(hi[part], look[2]) + dot_nn(low[part], look[0]) + dot_nn(mid[part], look[1])
            logits = logits + dot_nn(hi[part], look[1]) + dot_nn(mid[part], look[0]) + dot_nn(hi[part], look[0])
            halves.append(logits.T + offset)
        logits = jnp.concatenate(halves, axis=1)
        peak = jnp.max(logits, axis=0, keepdims=True)
        e = jnp.exp(logits - peak)
        expo[b] = e
        stat[b, 0:1, :] = peak
        stat[b, 1:2, :] = jnp.sum(e, axis=0, keepdims=True)
        if b == early - 1:
            pl.semaphore_wait(barrier, nz - 1 + ny - 1 + 1 + nx - 1)
            decay_mate.start()
            for ready in range(early):
                for copy in stats_to_peers(ready):
                    copy.start()
        if b >= early:
            for copy in stats_to_peers(b):
                copy.start()
    decay_mate.wait()
    decay0, decay1 = pair_decay[0], pair_decay[1]
    decay_y[y] = decay0 * decay1
    for k in spread(ny):
        to_y(k, decay_y.at[y], decay_y.at[y], decay_send.at[0], decay_recv.at[0]).start()

    half = kl // 2
    mass = jnp.zeros((kl, 1), jnp.float32)

    def moments(held, h, b):
        return [
            (coarse + dot_nn(wsplit[b, a], feat1[h, b]), fine + dot_nn(wsplit[b, a, 0:half, :], feat2[h, b]))
            for a, (coarse, fine) in enumerate(held)
        ]

    def nothing():
        return [(jnp.zeros((kl, width), jnp.float32), jnp.zeros((half, width), jnp.float32))] * 2

    def summed(held):
        return jnp.concatenate([fine + coarse[half:] + coarse[:half] for coarse, fine in held], axis=0)

    held = nothing()
    for b in range(blocks):
        if b % 2 == 0:
            for copy in stats_to_peers(b) + stats_to_peers(b + 1):
                copy.wait()
        near = stat[b, 0:1, :]
        peaks = [near] + [statin[k, b, 0:1, :] for k in range(nx - 1)]
        sums = [stat[b, 1:2, :]] + [statin[k, b, 1:2, :] for k in range(nx - 1)]
        peak = functools.reduce(jnp.maximum, peaks)
        whole = sum(s * jnp.exp(q - peak) for q, s in zip(peaks, sums))
        scale = jnp.exp(near - peak) / whole * wrow[b]
        w = expo[b] * scale
        mass = mass + jnp.sum(w, axis=1, keepdims=True)
        w1 = w.astype(jnp.bfloat16)
        w2 = (w - w1.astype(jnp.float32)).astype(jnp.bfloat16)
        for a in range(2):
            wsplit[b, a, 0:half, :] = w1[a * half : (a + 1) * half]
            wsplit[b, a, half:kl, :] = w2[a * half : (a + 1) * half]
        held = moments(held, 1 - c, b)
    other[...] = summed(held)
    other_mate = to_mate(other, partner, pair_send.at[1], pair_recv.at[1])
    other_mate.start()
    pair_mass[c] = row_of(mass)
    mass_mate = to_mate(pair_mass.at[c], pair_mass.at[c], pair_send.at[2], pair_recv.at[2])
    mass_mate.start()
    drain(decay_y.at[pl.ds(0, ny - 1)], decay_recv.at[0])
    decay_z[z] = decay_y[...]
    for k in spread(nz):
        to_z(k, decay_y, decay_z.at[z], decay_send.at[1], decay_recv.at[1]).start()
    held = nothing()
    for b in range(blocks):
        held = moments(held, c, b)
    acc = summed(held)
    mine[...] = acc
    other_mate.wait()

    first_core = c == 0
    lanes = width // PARTS

    def cut(h):
        return slice(h * lanes, (h + 1) * lanes)

    def thin(row):
        return row[:, 0:lanes]

    one = jnp.ones_like(decay0)
    combined = jnp.where(first_core, decay1, one) * acc + jnp.where(first_core, one, decay1) * partner[...]
    for h in range(PARTS):
        term[h] = combined[:, cut(h)]
        for k in spread(ny):
            to_y(k, term.at[h, band_rows(along_y(k))], terms.at[h, y], term_send.at[h], term_recv.at[h]).start()
        terms[h, y] = term[h, band_rows(y), :]
    mass_mate.wait()
    mass_y[y] = decay1 * pair_mass[0] + pair_mass[1]
    for k in spread(ny):
        to_y(k, mass_y.at[y], mass_y.at[y], mass_send.at[0], mass_recv.at[0]).start()
    mu_own, var_own = means[rows(y * nz + z), :], varis[rows(y * nz + z), :]
    start = mcol[rows(y * nz + z), 0:1] * jnp.where(first_core, mu_own, var_own + mu_own * mu_own)

    for h in range(PARTS):
        drain(terms.at[h, pl.ds(0, ny - 1)], term_recv.at[h])
        held = terms[h, 0]
        for q in range(1, ny):
            before[h, q] = held
            held = thin(decay_y[q]) * held + terms[h, q]
        plane[h] = held
        for k in spread(nz):
            to_z(k, plane.at[h, rows(along_z(k))], planes.at[h, z], plane_send.at[h], plane_recv.at[h]).start()
        planes[h, z] = plane[h, rows(z), :]
    drain(mass_y.at[pl.ds(0, ny - 1)], mass_recv.at[0])
    mass_z[z] = mass_y[...]
    for k in spread(nz):
        to_z(k, mass_y, mass_z.at[z], mass_send.at[1], mass_recv.at[1]).start()
    drain(decay_z.at[pl.ds(0, nz - 1)], decay_recv.at[1])
    plane_decay = [thin(functools.reduce(jnp.multiply, [decay_z[q, r] for r in range(ny)])) for q in range(nz)]

    for h in range(PARTS):
        drain(planes.at[h, pl.ds(0, nz - 1)], plane_recv.at[h])
        s = start[:, cut(h)]
        for q in range(nz):
            entry[h, q, 0] = s
            s = plane_decay[q] * s + planes[h, q]
        for q in range(nz):
            entry[h, q, 1] = s
        for k in spread(nz):
            to_z(k, entry.at[h, along_z(k)], entries.at[h, z], entry_send.at[h], entry_recv.at[h]).start()
        entries[h, z] = entry[h, z]

    drain(mass_z.at[pl.ds(0, nz - 1)], mass_recv.at[1])
    ms = mass_in[...]
    entry_mass = ms
    for q in range(nz):
        for r in range(ny):
            entry_mass = jnp.where(jnp.logical_and(q == z, r == y), ms, entry_mass)
            ms = decay_z[q, r] * ms + mass_z[q, r]
    mass0 = decay0 * entry_mass + pair_mass[0]
    mass1 = decay1 * mass0 + pair_mass[1]
    mass_row = jnp.where(first_core, mass0, mass1)
    dlog[...] = jnp.log(mass_row)
    flog[...] = jnp.log(ms)
    inv_dev[...] = jnp.broadcast_to(1.0 / column(mass_row), inv_dev.shape)
    inv_final[...] = jnp.broadcast_to(1.0 / column(ms), inv_final.shape)

    for h in range(PARTS):
        drain(entries.at[h, pl.ds(0, nz - 1)], entry_recv.at[h])
        carry, whole = entries[h, :, 0].reshape(band, lanes), entries[h, :, 1].reshape(band, lanes)
        ahead = thin(one)
        for q in range(ny):
            lines[h, q, 0] = ahead * carry + before[h, q] if q else carry
            lines[h, q, 1] = whole
            ahead = ahead * thin(decay_y[q])
        for k in spread(ny):
            to_y(k, lines.at[h, along_y(k)], linein.at[h, y], line_send.at[h], line_recv.at[h, k - 1]).start()
        linein[h, y] = lines[h, y]

    arrivals = [0] + sorted(range(1, ny), key=lambda k: min(k, ny - k))
    order = [(h, k) for h in range(PARTS) for k in arrivals]

    def from_band(k):
        return lax.rem(y - k + ny, ny)

    def band_to_mate(at, h, k):
        source = from_band(k)
        return (
            to_mate(linein.at[h, source, 1], total.at[h, source], chunk_send.at[2 * at], chunk_recv.at[2 * at]),
            to_mate(stateout.at[h, source], state.at[h, source], chunk_send.at[2 * at + 1], chunk_recv.at[2 * at + 1]),
        )

    for at, (h, k) in enumerate(order):
        source = from_band(k)
        if k:
            drain(linein.at[h, 0], line_recv.at[h, k - 1])
        total_mate, state_mate = band_to_mate(at, h, k)
        total_mate.start()
        from_own, from_mate = mine[band_rows(source), cut(h)], partner[band_rows(source), cut(h)]
        state0 = thin(decay0) * linein[h, source, 0] + jnp.where(first_core, from_own, from_mate)
        state1 = thin(decay1) * state0 + jnp.where(first_core, from_mate, from_own)
        stateout[h, source] = jnp.where(first_core, state1, state0)
        state_mate.start()
        mystate[h, source] = jnp.where(first_core, state0, state1)

    for at, (h, k) in enumerate(order):
        source = from_band(k)
        part = band_rows(source)
        total_mate, state_mate = band_to_mate(at, h, k)
        total_mate.wait()
        near, far = linein[h, source, 1], total[h, source]
        scale = inv_final[part, 0:1]
        centers = jnp.where(first_core, near, far) * scale
        fmean[part, cut(h)] = centers
        fvar[part, cut(h)] = jnp.where(first_core, far, near) * scale - centers * centers + VAR_PRIOR
        state_mate.wait()
        near, far = mystate[h, source], state[h, source]
        scale = inv_dev[part, 0:1]
        centers = jnp.where(first_core, near, far) * scale
        dmean[part, cut(h)] = centers
        dvar[part, cut(h)] = jnp.where(first_core, far, near) * scale - centers * centers + VAR_PRIOR

    for h in range(PARTS):
        drain(terms.at[h, pl.ds(0, ny - 1)], term_send.at[h])
        drain(planes.at[h, pl.ds(0, nz - 1)], plane_send.at[h])
        drain(entries.at[h, pl.ds(0, nz - 1)], entry_send.at[h])
        drain(linein.at[h, pl.ds(0, ny - 1)], line_send.at[h])
    drain(decay_y.at[pl.ds(0, ny - 1)], decay_send.at[0])
    drain(decay_z.at[pl.ds(0, nz - 1)], decay_send.at[1])
    drain(mass_y.at[pl.ds(0, ny - 1)], mass_send.at[0])
    drain(mass_z.at[pl.ds(0, nz - 1)], mass_send.at[1])


def deliver(*refs):
    copies = [pltpu.make_async_copy(refs[k], refs[6 + k], refs[12].at[k]) for k in range(6)]
    for copy in copies:
        copy.start()
    for copy in copies:
        copy.wait()


def local(nz, ny, nx, points, assign, plan, init_mass, init_means, init_vars):
    kl, width = init_means.shape
    count = points.shape[0]
    nc, blocks = nz * ny, count // BLOCK
    share, band, lanes = kl // nc, kl // ny, width // PARTS
    f32, bf16 = jnp.float32, jnp.bfloat16
    vmem, hbm, dma = pltpu.VMEM, pltpu.HBM, pltpu.SemaphoreType.DMA
    row, table = jax.ShapeDtypeStruct((1, kl), f32), jax.ShapeDtypeStruct((kl, width), f32)
    far = functools.partial(pltpu.with_memory_space_constraint, memory_space=hbm)
    outs = pl.pallas_call(
        functools.partial(kernel, nz, ny, nx),
        out_shape=(row, table, table, row, table, table),
        in_specs=[pl.BlockSpec(memory_space=hbm)] * 6,
        out_specs=[pl.BlockSpec(memory_space=vmem)] * 6,
        scratch_shapes=[
            vmem((blocks, BLOCK, width), f32),
            vmem((kl, width), f32),
            vmem((kl, width), f32),
            vmem((1, count), jnp.int32),
            vmem(plan.shape, jnp.int32),
            vmem((1, kl), f32),
            dma((5 + blocks,)),
            vmem((3, 2 * width, kl), bf16),
            vmem((2, blocks, BLOCK, width), bf16),
            vmem((2, blocks, BLOCK, width), bf16),
            vmem((blocks, kl, BLOCK), f32),
            vmem((blocks, 2, kl, BLOCK), bf16),
            vmem((blocks, 1, BLOCK), f32),
            vmem((kl, 128), f32),
            vmem((blocks, 2, BLOCK), f32),
            vmem((nx - 1, blocks, 2, BLOCK), f32),
            vmem((kl, width), f32),
            vmem((kl, width), f32),
            vmem((kl, width), f32),
            vmem((2, 1, kl), f32),
            vmem((2, 1, kl), f32),
            vmem((ny, 1, kl), f32),
            vmem((nz, ny, 1, kl), f32),
            vmem((ny, 1, kl), f32),
            vmem((nz, ny, 1, kl), f32),
            vmem((PARTS, kl, lanes), f32),
            vmem((PARTS, ny, band, lanes), f32),
            vmem((PARTS, ny, band, lanes), f32),
            vmem((PARTS, band, lanes), f32),
            vmem((PARTS, nz, share, lanes), f32),
            vmem((PARTS, nz, 2, share, lanes), f32),
            vmem((PARTS, nz, 2, share, lanes), f32),
            vmem((PARTS, ny, 2, band, lanes), f32),
            vmem((PARTS, ny, 2, band, lanes), f32),
            vmem((PARTS, ny, band, lanes), f32),
            vmem((PARTS, ny, band, lanes), f32),
            vmem((PARTS, ny, band, lanes), f32),
            vmem((PARTS, ny, band, lanes), f32),
            vmem((kl, 128), f32),
            vmem((kl, 128), f32),
            dma((nx - 1, blocks)), dma((nx - 1, blocks)),
            dma((3,)), dma((3,)),
            dma((PARTS,)), dma((PARTS,)), dma((PARTS,)), dma((PARTS,)), dma((PARTS,)), dma((PARTS,)),
            dma((PARTS,)), dma((PARTS, ny - 1)), dma((2,)), dma((2,)), dma((2,)), dma((2,)),
            dma((2 * PARTS * ny,)), dma((2 * PARTS * ny,)),
        ],
        compiler_params=pltpu.CompilerParams(collective_id=0, has_side_effects=True, vmem_limit_bytes=32 * 2**20),
    )(*(far(a) for a in (points, assign, plan, init_mass.reshape(1, kl), init_means, init_vars)))
    outs = pl.pallas_call(
        deliver,
        out_shape=tuple(jax.ShapeDtypeStruct(o.shape, f32) for o in outs),
        in_specs=[pl.BlockSpec(memory_space=vmem)] * 6,
        out_specs=[pl.BlockSpec(memory_space=hbm)] * 6,
        scratch_shapes=[dma((6,))],
        compiler_params=pltpu.CompilerParams(vmem_limit_bytes=2 * 2**20),
    )(*outs)
    return tuple(o.reshape(1, kl) if o.shape[0] == 1 else o[None] for o in outs)


def solution(mesh):
    nz, ny, nx = 8, 4, mesh.shape["comp"]
    split = Mesh(mesh.devices.reshape(nz, ny, 2, nx), (*SEQ, "comp"))
    return jax.shard_map(
        functools.partial(local, nz, ny, nx),
        mesh=split,
        in_specs=(P(SEQ, None), P(SEQ, None), P(SEQ, None), P("comp"), P("comp", None), P("comp", None)),
        out_specs=(
            P(SEQ, "comp"), P(SEQ, "comp", None), P(SEQ, "comp", None),
            P(SEQ, "comp"), P(SEQ, "comp", None), P(SEQ, "comp", None),
        ),
        check_vma=False,
    )
```
